128 devices in a mesh: tok: 8 (over z, core), head: 16 (over x, y).
Axes of the slice: x: 4, y: 4, z: 4, core: 2. Of those that a mesh axis runs over, the one named last changes fastest.
Arguments:
- queries: bfloat16 [4096, 16384], P('tok', 'head'), may hold values from -9 to 9
- keys: bfloat16 [4096, 1024], P('tok'), may hold values from -6 to 6
- values: bfloat16 [4096, 1024], P('tok'), may hold values from -6 to 6
- grad_out: bfloat16 [4096, 16384], P('tok', 'head'), may hold values from -6 to 6
- doc_ids: int32 [4096], P('tok'), may hold values from 0 to 5, never falling along the last dimension, each value on 1 to 2048 neighbouring positions
Outputs:
- attn_out: bfloat16 [4096, 16384], P('tok', 'head')
- grad_queries: bfloat16 [4096, 16384], P('tok', 'head')
- grad_keys: bfloat16 [4096, 1024], P(('tok', 'head'))
- grad_values: bfloat16 [4096, 1024], P(('tok', 'head'))
The draws below stay inside these ranges and needn't reach their ends.
All inputs are finite; a program needn't handle non-finite values.
Results may differ from the reference program's by a relative error of at most 0.04.
Values may be sent and summed in bfloat16 or wider, within the bound.
A program may use at most 64 MiB of HBM per device.

```python
import math
import jax
import jax.numpy as jnp
import numpy as np
from jax import lax

H = 128
KVH = 8
HD = 128
DOCS = 6
TOKENS = 4096


def draw_queries(key, part):
    drawn = jnp.clip(jax.random.normal(jax.random.fold_in(key, 21), (TOKENS, H * HD), jnp.float32), -6.0, 6.0)
    return drawn.astype(jnp.bfloat16)


def draw_keys(key, part):
    drawn = jnp.clip(jax.random.normal(jax.random.fold_in(key, 22), (TOKENS, KVH * HD), jnp.float32), -6.0, 6.0)
    return drawn.astype(jnp.bfloat16)


def block_levels(rng, extent, split, smallest, high):
    gain, own = 1.0, jax.random.fold_in(rng, 6)
    for dim, shards_of in split:
        steps = jnp.exp(jax.random.uniform(jax.random.fold_in(own, dim), (shards_of,), jnp.float32, smallest / len(split), high / len(split)))
        gain = gain * jnp.repeat(steps, extent[dim] // shards_of).reshape([-1 if axis == dim else 1 for axis in range(len(extent))])
    return gain


def length_profile(amount, total, most, skew):
    loads = [(1 << 20) // math.isqrt(standing ** skew) + 1 for standing in range(2, amount + 1)]
    rest, holding = total - most - (amount - 1), [1] * (amount - 1)
    while rest > 0:
        movable = [i for i in range(amount - 1) if holding[i] < most]
        mass, budget = sum([loads[i] for i in movable]), rest
        for i in movable:
            more = min(most - holding[i], max(1, budget * loads[i] // mass), rest)
            holding[i] = holding[i] + more
            rest = rest - more
    return np.array([most] + holding)


def ragged_sizes(stream_key, number_of, total, limit, slope):
    if number_of == 2:
        one = jax.random.randint(stream_key, (), max(1, total - limit), min(limit, total - 1) + 1)
        return jnp.stack([one, total - one])
    tallies = jnp.asarray(length_profile(number_of, total, limit, slope), jnp.int32)
    pairs = (number_of - 1) // 2
    giver, receiver = tallies[1:1 + 2 * pairs:2], tallies[2:2 + 2 * pairs:2]
    slack = jnp.minimum(giver - 1, limit - receiver)
    moved = jax.random.randint(jax.random.fold_in(stream_key, 1), (pairs,), 0, 1 << 20) % (slack + 1)
    tallies = tallies.at[1:1 + 2 * pairs:2].set(giver - moved).at[2:2 + 2 * pairs:2].set(receiver + moved)
    return tallies[jax.random.permutation(jax.random.fold_in(stream_key, 2), number_of)]


def noise(own_key, dims, scale, most, pieces=(), kind=jnp.bfloat16):
    result = scale * jax.random.normal(own_key, dims, jnp.float32)
    if pieces:
        result = result * block_levels(own_key, dims, pieces, -0.22, 0.18)
    return jnp.clip(result, -most, most).astype(kind)


def setup_inputs(seed: int = 0) -> dict:
    key_of = jax.random.split(jax.random.key(seed), 6)
    return {
        "queries": draw_queries(jax.random.fold_in(key_of[5], 71), 0),
        "keys": draw_keys(jax.random.fold_in(key_of[5], 71), 0),
        "values": noise(key_of[2], (TOKENS, KVH * HD), 1.0, 6.0, ((0, 8),)),
        "grad_out": noise(key_of[3], (TOKENS, H * HD), 1.0, 6.0, ((0, 8), (1, 16))),
        "doc_ids": jnp.searchsorted(jnp.cumsum(ragged_sizes(key_of[4], DOCS, TOKENS, TOKENS // 2, 1)), jnp.arange(TOKENS), side="right").astype(jnp.int32),
    }


def reference(queries, keys, values, grad_out, doc_ids):
    score_scale = HD ** -0.5
    group_size = H // KVH
    positions = jnp.arange(TOKENS, dtype=jnp.int32)
    allowed = (doc_ids[None, :] == doc_ids[:, None]) & (positions[None, :] <= positions[:, None])

    def one_head(head_number):
        kv_head = head_number // group_size
        query_h = lax.dynamic_slice_in_dim(queries, head_number * HD, HD, 1)
        grad_h = lax.dynamic_slice_in_dim(grad_out, head_number * HD, HD, 1)
        key_g = lax.dynamic_slice_in_dim(keys, kv_head * HD, HD, 1)
        value_g = lax.dynamic_slice_in_dim(values, kv_head * HD, HD, 1)
        scores = jnp.dot(query_h, key_g.T, preferred_element_type=jnp.float32) * score_scale
        scores = jnp.where(allowed, scores, -1e30)
        row_max = jnp.max(scores, axis=1)
        log_total = row_max + jnp.log(jnp.sum(jnp.exp(scores - row_max[:, None]), axis=1))
        probs = jnp.where(allowed, jnp.exp(scores - log_total[:, None]), 0.0)
        probs_low = probs.astype(jnp.bfloat16)
        output_f = jnp.dot(probs_low, value_g, preferred_element_type=jnp.float32)
        row_delta = jnp.sum(grad_h.astype(jnp.float32) * output_f, axis=1)
        grad_probs = jnp.dot(grad_h, value_g.T, preferred_element_type=jnp.float32)
        grad_scores = (probs * (grad_probs - row_delta[:, None])).astype(jnp.bfloat16)
        grad_query = jnp.dot(grad_scores, key_g, preferred_element_type=jnp.float32) * score_scale
        grad_key = jnp.dot(grad_scores.T, query_h, preferred_element_type=jnp.float32) * score_scale
        grad_value = jnp.dot(probs_low.T, grad_h, preferred_element_type=jnp.float32)
        return output_f.astype(jnp.bfloat16), grad_query.astype(jnp.bfloat16), grad_key, grad_value

    outputs, grad_qs, grad_ks, grad_vs = lax.map(one_head, jnp.arange(H, dtype=jnp.int32))
    attn_out = outputs.transpose(1, 0, 2).reshape(TOKENS, H * HD)
    grad_queries = grad_qs.transpose(1, 0, 2).reshape(TOKENS, H * HD)
    grad_keys = grad_ks.reshape(KVH, group_size, TOKENS, HD).sum(axis=1)
    grad_values = grad_vs.reshape(KVH, group_size, TOKENS, HD).sum(axis=1)
    grad_keys = grad_keys.transpose(1, 0, 2).reshape(TOKENS, KVH * HD).astype(jnp.bfloat16)
    grad_values = grad_values.transpose(1, 0, 2).reshape(TOKENS, KVH * HD).astype(jnp.bfloat16)
    return attn_out, grad_queries, grad_keys, grad_values
```

```python
import math

import jax
import jax.numpy as jnp
from jax import lax
from jax.experimental import pallas as pl
from jax.experimental.pallas import tpu as pltpu
from jax.sharding import PartitionSpec as P

KVH = 8
HD = 128
T = 256
REACH = 8
NT = REACH + 1
BIG = -131072.0
SCALE = HD**-0.5
EXP2_SCALE = SCALE * math.log2(math.e)
NEG = -1e30


def nt(a, b):
    return lax.dot_general(a, b, (((1,), (1,)), ((), ())), preferred_element_type=jnp.float32)


def nn(a, b):
    return lax.dot_general(a, b, (((1,), (0,)), ((), ())), preferred_element_type=jnp.float32)


def attend_kernel(
    q_ref, g_ref, k_ref, v_ref, e_ref, b_ref,
    out_ref, dq_ref, dkv_ref,
    kt_ref, vt_ref, s_ref, p_ref, ds_ref, dk_ref, dv_ref,
):
    tiles = k_ref.shape[0]
    heads = q_ref.shape[1] // HD

    def transpose_step(i, _):
        kt_ref[i] = k_ref[i].T
        vt_ref[i] = v_ref[i].T
        dk_ref[i] = jnp.zeros((T, HD), jnp.float32)
        dv_ref[i] = jnp.zeros((T, HD), jnp.float32)
        return 0

    lax.fori_loop(0, tiles, transpose_step, 0)

    key_pos = lax.broadcasted_iota(jnp.int32, (T, T), 0)
    row_pos = lax.broadcasted_iota(jnp.int32, (T, T), 1)

    def step(i, _):
        rb = i // heads
        h = i % heads
        rows = pl.ds(pl.multiple_of(rb * T, T), T)
        cols = pl.ds(pl.multiple_of(h * HD, HD), HD)
        q = q_ref[rows, cols]
        g = g_ref[rows, cols]
        q_ext = jnp.concatenate([q, b_ref[rows, :]], axis=1)
        gt = g.astype(jnp.float32).T
        top = jnp.full((8, T), NEG, jnp.float32)
        for j in range(NT):
            k_ext = jnp.concatenate([k_ref[rb + j], e_ref[rb + j]], axis=1)
            s = nt(k_ext, q_ext)
            if j == NT - 1:
                s = jnp.where(key_pos <= row_pos, s, BIG)
            s_ref[j] = s
            top = jnp.maximum(top, jnp.max(s.reshape(T // 8, 8, T), axis=0))
        top = jnp.max(top, axis=0, keepdims=True) * EXP2_SCALE
        total = jnp.zeros((8, T), jnp.float32)
        ot = jnp.zeros((HD, T), jnp.float32)
        for j in range(NT):
            p = jnp.exp2(s_ref[j] * EXP2_SCALE - top)
            total = total + jnp.sum(p.reshape(T // 8, 8, T), axis=0)
            pb = p.astype(jnp.bfloat16)
            p_ref[j] = pb
            ot = ot + nn(vt_ref[rb + j], pb)
        inverse = 1.0 / jnp.sum(total, axis=0, keepdims=True)
        ot = ot * inverse
        out_ref[rows, cols] = ot.T.astype(jnp.bfloat16)
        gn = (gt * inverse).astype(jnp.bfloat16)
        delta = jnp.sum(gn.astype(jnp.float32) * ot, axis=0, keepdims=True)
        dqt = jnp.zeros((HD, T), jnp.float32)
        for j in range(NT):
            dp = nn(v_ref[rb + j], gn)
            pb = p_ref[j]
            ds = (dp - delta).astype(jnp.bfloat16) * pb
            dqt = dqt + nn(kt_ref[rb + j], ds)
            dk_ref[rb + j] += nn(ds, q)
            dv_ref[rb + j] += nt(pb, gn)
        dq_ref[rows, cols] = (dqt * SCALE).T.astype(jnp.bfloat16)
        return 0

    lax.fori_loop(0, (q_ref.shape[0] // T) * heads, step, 0)

    def finish(i, _):
        dkv_ref[i, :, 0:HD] = (dk_ref[i] * SCALE).astype(jnp.bfloat16)
        dkv_ref[i, :, HD : 2 * HD] = dv_ref[i].astype(jnp.bfloat16)
        return 0

    lax.fori_loop(0, tiles, finish, 0)


def attend(q, g, k, v, e, b):
    tiles = k.shape[0]
    rows, width = q.shape
    pairs = (rows // T) * NT * T * T * (width // HD)
    return pl.pallas_call(
        attend_kernel,
        out_shape=(
            jax.ShapeDtypeStruct((rows, width), jnp.bfloat16),
            jax.ShapeDtypeStruct((rows, width), jnp.bfloat16),
            jax.ShapeDtypeStruct((tiles, T, 2 * HD), jnp.bfloat16),
        ),
        in_specs=[pl.BlockSpec(memory_space=pltpu.VMEM)] * 6,
        out_specs=[pl.BlockSpec(memory_space=pltpu.VMEM)] * 3,
        scratch_shapes=[
            pltpu.VMEM((tiles, HD, T), jnp.bfloat16),
            pltpu.VMEM((tiles, HD, T), jnp.bfloat16),
            pltpu.VMEM((NT, T, T), jnp.float32),
            pltpu.VMEM((NT, T, T), jnp.bfloat16),
            pltpu.VMEM((NT, T, T), jnp.bfloat16),
            pltpu.VMEM((tiles, T, HD), jnp.float32),
            pltpu.VMEM((tiles, T, HD), jnp.float32),
        ],
        compiler_params=pltpu.CompilerParams(vmem_limit_bytes=48 * 1024 * 1024),
        cost_estimate=pl.CostEstimate(
            flops=pairs * 12 * HD, bytes_accessed=rows * width * 8, transcendentals=pairs
        ),
    )(q, g, k, v, e, b)


def body(queries, keys, values, grad_out, doc_ids):
    tok_count = lax.axis_size("tok")
    head_count = lax.axis_size("head")
    tok_number = lax.axis_index("tok")
    head_number = lax.axis_index("head")
    rows = queries.shape[0]
    copies = head_count // KVH
    group = head_number // copies
    span = REACH * T
    key_own = lax.dynamic_slice_in_dim(keys, group * HD, HD, 1)
    value_own = lax.dynamic_slice_in_dim(values, group * HD, HD, 1)
    docs_own = doc_ids.astype(jnp.bfloat16)[:, None]
    packed = jnp.concatenate([key_own, value_own, docs_own], axis=1)
    gathered = lax.all_gather(packed, "tok", axis=0, tiled=True)
    padded = jnp.pad(gathered, ((span, 0), (0, 0)))
    local = lax.dynamic_slice_in_dim(padded, tok_number * rows, span + rows, 0)
    tiles = (span + rows) // T
    k = local[:, 0:HD].reshape(tiles, T, HD)
    v = local[:, HD : 2 * HD].reshape(tiles, T, HD)
    positions = tok_number * rows - span + jnp.arange(span + rows)
    docs = jnp.where(positions >= 0, local[:, 2 * HD].astype(jnp.int32), 6)
    lanes = jnp.arange(HD)[None, :]
    e = (docs[:, None] == lanes).astype(jnp.bfloat16).reshape(tiles, T, HD)
    b = jnp.where(doc_ids[:, None] == lanes, 0.0, BIG).astype(jnp.bfloat16)
    attn_out, grad_queries, dkv = attend(queries, grad_out, k, v, e, b)
    dkv = dkv.reshape(span + rows, 2 * HD)
    whole = jnp.zeros((span + tok_count * rows, 2 * HD), jnp.bfloat16)
    whole = lax.dynamic_update_slice_in_dim(whole, dkv, tok_number * rows, 0)[span:]
    mine = lax.psum_scatter(whole, "tok", scatter_dimension=0, tiled=True)
    piece = rows // head_count
    spread = lax.all_to_all(
        mine.reshape(head_count, piece, 2 * HD), "head", split_axis=0, concat_axis=0, tiled=True
    )
    final = spread.astype(jnp.float32).reshape(KVH, copies, piece, 2 * HD).sum(axis=1)
    final = final.astype(jnp.bfloat16).transpose(1, 0, 2)
    return (
        attn_out,
        grad_queries,
        final[:, :, :HD].reshape(piece, KVH * HD),
        final[:, :, HD:].reshape(piece, KVH * HD),
    )


def solution(mesh):
    return jax.shard_map(
        body,
        mesh=mesh,
        in_specs=(P("tok", "head"), P("tok", None), P("tok", None), P("tok", "head"), P("tok")),
        out_specs=(
            P("tok", "head"),
            P("tok", "head"),
            P(("tok", "head"), None),
            P(("tok", "head"), None),
        ),
        check_vma=False,
    )
```

```python
import math

import jax
import jax.numpy as jnp
from jax import lax
from jax.experimental import pallas as pl
from jax.experimental.pallas import tpu as pltpu
from jax.sharding import PartitionSpec as P

KVH = 8
HD = 128
T = 256
REACH = 8
NT = REACH + 1
BIG = -131072.0
SCALE = HD**-0.5
EXP2_SCALE = SCALE * math.log2(math.e)
NEG = -1e30


def nt(a, b):
    return lax.dot_general(a, b, (((1,), (1,)), ((), ())), preferred_element_type=jnp.float32)


def nn(a, b):
    return lax.dot_general(a, b, (((1,), (0,)), ((), ())), preferred_element_type=jnp.float32)


def attend_kernel(
    q_ref, g_ref, kv_ref, docs_ref,
    out_ref, dq_ref, dkv_ref,
    ke_ref, kt_ref, vt_ref, b_ref, s_ref, p_ref, ds_ref, dk_ref, dv_ref,
):
    tiles = ke_ref.shape[0]
    per_block = kv_ref.shape[1] // T
    heads = q_ref.shape[1] // HD
    half = T // HD
    kinds = lax.broadcasted_iota(jnp.int32, (HD, HD), 0)

    def prepare(i, _):
        block = i // per_block
        part = i % per_block
        rows = pl.ds(pl.multiple_of(part * T, T), T)
        key = kv_ref[block, rows, 0:HD]
        kt_ref[i] = key.T
        vt_ref[i] = kv_ref[block, rows, HD : 2 * HD].T
        ke_ref[i, :, 0:HD] = key
        for r in range(half):
            docs = docs_ref[block, pl.ds(part * half + r, 1), :]
            hot = jnp.where(docs == kinds, 1.0, 0.0)
            ke_ref[i, r * HD : (r + 1) * HD, HD : 2 * HD] = hot.T.astype(jnp.bfloat16)
        dk_ref[i] = jnp.zeros((T, HD), jnp.float32)
        dv_ref[i] = jnp.zeros((T, HD), jnp.float32)
        return 0

    lax.fori_loop(0, tiles, prepare, 0)
    last = kv_ref.shape[0] - 1
    for r in range(b_ref.shape[0] // HD):
        docs = docs_ref[last, r : r + 1, :]
        cold = jnp.where(docs == kinds, 0.0, BIG)
        b_ref[r * HD : (r + 1) * HD, :] = cold.T.astype(jnp.bfloat16)

    key_pos = lax.broadcasted_iota(jnp.int32, (T, T), 0)
    row_pos = lax.broadcasted_iota(jnp.int32, (T, T), 1)

    def step(i, _):
        rb = i // heads
        h = i % heads
        rows = pl.ds(pl.multiple_of(rb * T, T), T)
        cols = pl.ds(pl.multiple_of(h * HD, HD), HD)
        q = q_ref[rows, cols]
        g = g_ref[rows, cols]
        q_ext = jnp.concatenate([q, b_ref[rows, :]], axis=1)
        gt = g.astype(jnp.float32).T
        top = jnp.full((8, T), NEG, jnp.float32)
        for j in range(NT):
            s = nt(ke_ref[rb + j], q_ext)
            if j == NT - 1:
                s = jnp.where(key_pos <= row_pos, s, BIG)
            s_ref[j] = s
            top = jnp.maximum(top, jnp.max(s.reshape(T // 8, 8, T), axis=0))
        top = jnp.max(top, axis=0, keepdims=True) * EXP2_SCALE
        total = jnp.zeros((8, T), jnp.float32)
        ot = jnp.zeros((HD, T), jnp.float32)
        for j in range(NT):
            p = jnp.exp2(s_ref[j] * EXP2_SCALE - top)
            total = total + jnp.sum(p.reshape(T // 8, 8, T), axis=0)
            pb = p.astype(jnp.bfloat16)
            p_ref[j] = pb
            ot = ot + nn(vt_ref[rb + j], pb)
        inverse = 1.0 / jnp.sum(total, axis=0, keepdims=True)
        ot = ot * inverse
        out_ref[rows, cols] = ot.T.astype(jnp.bfloat16)
        gn = (gt * inverse).astype(jnp.bfloat16)
        delta = jnp.sum(gn.astype(jnp.float32) * ot, axis=0, keepdims=True)
        dqt = jnp.zeros((HD, T), jnp.float32)
        for j in range(NT):
            block = (rb + j) // per_block
            part = (rb + j) % per_block
            v = kv_ref[block, pl.ds(pl.multiple_of(part * T, T), T), HD : 2 * HD]
            dp = nn(v, gn)
            pb = p_ref[j]
            ds = (dp - delta).astype(jnp.bfloat16) * pb
            dqt = dqt + nn(kt_ref[rb + j], ds)
            dk_ref[rb + j] += nn(ds, q)
            dv_ref[rb + j] += nt(pb, gn)
        dq_ref[rows, cols] = (dqt * SCALE).T.astype(jnp.bfloat16)
        return 0

    lax.fori_loop(0, (q_ref.shape[0] // T) * heads, step, 0)

    def finish(i, _):
        rows = pl.ds(pl.multiple_of((i % per_block) * T, T), T)
        dkv_ref[i // per_block, rows, 0:HD] = (dk_ref[i] * SCALE).astype(jnp.bfloat16)
        dkv_ref[i // per_block, rows, HD : 2 * HD] = dv_ref[i].astype(jnp.bfloat16)
        return 0

    lax.fori_loop(0, tiles, finish, 0)


def attend(q, g, kv, docs):
    blocks, rows, _ = kv.shape
    tiles = blocks * rows // T
    width = q.shape[1]
    pairs = (rows // T) * NT * T * T * (width // HD)
    return pl.pallas_call(
        attend_kernel,
        out_shape=(
            jax.ShapeDtypeStruct((rows, width), jnp.bfloat16),
            jax.ShapeDtypeStruct((rows, width), jnp.bfloat16),
            jax.ShapeDtypeStruct((blocks, rows, 2 * HD), jnp.bfloat16),
        ),
        in_specs=[pl.BlockSpec(memory_space=pltpu.VMEM)] * 4,
        out_specs=[pl.BlockSpec(memory_space=pltpu.VMEM)] * 3,
        scratch_shapes=[
            pltpu.VMEM((tiles, T, 2 * HD), jnp.bfloat16),
            pltpu.VMEM((tiles, HD, T), jnp.bfloat16),
            pltpu.VMEM((tiles, HD, T), jnp.bfloat16),
            pltpu.VMEM((rows, HD), jnp.bfloat16),
            pltpu.VMEM((NT, T, T), jnp.float32),
            pltpu.VMEM((NT, T, T), jnp.bfloat16),
            pltpu.VMEM((NT, T, T), jnp.bfloat16),
            pltpu.VMEM((tiles, T, HD), jnp.float32),
            pltpu.VMEM((tiles, T, HD), jnp.float32),
        ],
        compiler_params=pltpu.CompilerParams(vmem_limit_bytes=48 * 1024 * 1024),
        cost_estimate=pl.CostEstimate(
            flops=pairs * 12 * HD, bytes_accessed=rows * width * 8, transcendentals=pairs
        ),
        name="attend",
    )(q, g, kv, docs)


def greet(peers):
    barrier = pltpu.get_barrier_semaphore()
    for peer in peers:
        pl.semaphore_signal(
            barrier, inc=1, device_id=peer, device_id_type=pl.DeviceIdType.MESH
        )
    pl.semaphore_wait(barrier, len(peers))


def others(axis):
    count = lax.axis_size(axis)
    me = lax.axis_index(axis)
    return [{axis: lax.rem(me + d, count)} for d in range(1, count)]


def gather_kernel(
    keys_ref, values_ref, docs_ref, kv_ref, all_docs_ref, load_sems, send_sems, recv_sems
):
    tok = lax.axis_index("tok")
    toks = lax.axis_size("tok")
    group = lax.axis_index("head") // (lax.axis_size("head") // KVH)
    blocks = kv_ref.shape[0]
    last = blocks - 1
    cols = pl.ds(pl.multiple_of(group * HD, HD), HD)
    loads = [
        pltpu.make_async_copy(keys_ref.at[:, cols], kv_ref.at[last, :, 0:HD], load_sems.at[0]),
        pltpu.make_async_copy(
            values_ref.at[:, cols], kv_ref.at[last, :, HD : 2 * HD], load_sems.at[1]
        ),
    ]
    for load in loads:
        load.start()
    all_docs_ref[last] = docs_ref[...]
    greet(others("tok"))
    for load in loads:
        load.wait()

    def copies(d, peer):
        return [
            pltpu.make_async_remote_copy(
                src_ref=kv_ref.at[last],
                dst_ref=kv_ref.at[last - d],
                send_sem=send_sems.at[0, d - 1],
                recv_sem=recv_sems.at[0, d - 1],
                device_id={"tok": peer},
                device_id_type=pl.DeviceIdType.MESH,
            ),
            pltpu.make_async_remote_copy(
                src_ref=docs_ref,
                dst_ref=all_docs_ref.at[last - d],
                send_sem=send_sems.at[1, d - 1],
                recv_sem=recv_sems.at[1, d - 1],
                device_id={"tok": peer},
                device_id_type=pl.DeviceIdType.MESH,
            ),
        ]

    for d in range(1, blocks):

        @pl.when(tok + d < toks)
        def _():
            for copy in copies(d, tok + d):
                copy.start()

        @pl.when(tok < d)
        def _():
            kv_ref[last - d] = jnp.zeros(kv_ref.shape[1:], jnp.bfloat16)
            all_docs_ref[last - d] = jnp.full(docs_ref.shape, 6, jnp.int32)

    for d in range(1, blocks):

        @pl.when(tok + d < toks)
        def _():
            for copy in copies(d, tok + d):
                copy.wait_send()

        @pl.when(tok >= d)
        def _():
            for copy in copies(d, tok - d):
                copy.wait_recv()


def gather(keys, values, docs, blocks):
    rows = keys.shape[0]
    vmem = pl.BlockSpec(memory_space=pltpu.VMEM)
    hbm = pl.BlockSpec(memory_space=pl.ANY)
    return pl.pallas_call(
        gather_kernel,
        out_shape=(
            jax.ShapeDtypeStruct((blocks, rows, 2 * HD), jnp.bfloat16),
            jax.ShapeDtypeStruct((blocks,) + docs.shape, jnp.int32),
        ),
        in_specs=[hbm, hbm, vmem],
        out_specs=[vmem, vmem],
        scratch_shapes=[
            pltpu.SemaphoreType.DMA((2,)),
            pltpu.SemaphoreType.DMA((2, blocks - 1)),
            pltpu.SemaphoreType.DMA((2, blocks - 1)),
        ],
        compiler_params=pltpu.CompilerParams(collective_id=0, has_side_effects=True),
        name="gather",
    )(keys, values, docs)


def reduce_kernel(
    dkv_ref, dk_ref, dv_ref, terms_ref, mid_ref, parts_ref, send_sems, recv_sems, out_sems, in_sems
):
    tok = lax.axis_index("tok")
    toks = lax.axis_size("tok")
    head = lax.axis_index("head")
    head_count = lax.axis_size("head")
    blocks = dkv_ref.shape[0]
    last = blocks - 1
    piece = mid_ref.shape[1]
    greet(others("tok") + others("head"))

    def term(d, peer):
        return pltpu.make_async_remote_copy(
            src_ref=dkv_ref.at[last - d],
            dst_ref=terms_ref.at[d - 1],
            send_sem=send_sems.at[d - 1],
            recv_sem=recv_sems.at[d - 1],
            device_id={"tok": peer},
            device_id_type=pl.DeviceIdType.MESH,
        )

    for d in range(1, blocks):

        @pl.when(tok >= d)
        def _():
            term(d, tok - d).start()

        @pl.when(tok + d >= toks)
        def _():
            terms_ref[d - 1] = jnp.zeros(terms_ref.shape[1:], jnp.bfloat16)

    for d in range(1, blocks):

        @pl.when(tok + d < toks)
        def _():
            term(d, tok + d).wait_recv()

    def add(i, _):
        rows = pl.ds(pl.multiple_of(i * piece, piece), piece)
        total = dkv_ref[last, rows, :].astype(jnp.float32)
        for d in range(1, blocks):
            total = total + terms_ref[d - 1, rows, :].astype(jnp.float32)
        mid_ref[i] = total.astype(jnp.bfloat16)
        return 0

    lax.fori_loop(0, head_count, add, 0)

    def part(d, peer, slot):
        return pltpu.make_async_remote_copy(
            src_ref=mid_ref.at[peer],
            dst_ref=parts_ref.at[slot],
            send_sem=out_sems.at[d - 1],
            recv_sem=in_sems.at[d - 1],
            device_id={"head": peer},
            device_id_type=pl.DeviceIdType.MESH,
        )

    for d in range(1, head_count):
        part(d, lax.rem(head + d, head_count), head).start()
    parts_ref[head] = mid_ref[head]
    for d in range(1, head_count):
        source = lax.rem(head + head_count - d, head_count)
        part(d, source, source).wait_recv()
    copies = head_count // KVH
    for g in range(KVH):
        total = parts_ref[g * copies].astype(jnp.float32)
        for c in range(1, copies):
            total = total + parts_ref[g * copies + c].astype(jnp.float32)
        total = total.astype(jnp.bfloat16)
        dk_ref[:, g * HD : (g + 1) * HD] = total[:, 0:HD]
        dv_ref[:, g * HD : (g + 1) * HD] = total[:, HD : 2 * HD]
    for d in range(1, blocks):

        @pl.when(tok >= d)
        def _():
            term(d, tok - d).wait_send()

    for d in range(1, head_count):
        part(d, lax.rem(head + d, head_count), head).wait_send()


def reduce(dkv, head_count):
    blocks, rows, width = dkv.shape
    piece = rows // head_count
    vmem = pl.BlockSpec(memory_space=pltpu.VMEM)
    return pl.pallas_call(
        reduce_kernel,
        out_shape=(jax.ShapeDtypeStruct((piece, KVH * HD), jnp.bfloat16),) * 2,
        in_specs=[vmem],
        out_specs=[vmem, vmem],
        scratch_shapes=[
            pltpu.VMEM((blocks - 1, rows, width), jnp.bfloat16),
            pltpu.VMEM((head_count, piece, width), jnp.bfloat16),
            pltpu.VMEM((head_count, piece, width), jnp.bfloat16),
            pltpu.SemaphoreType.DMA((blocks - 1,)),
            pltpu.SemaphoreType.DMA((blocks - 1,)),
            pltpu.SemaphoreType.DMA((head_count - 1,)),
            pltpu.SemaphoreType.DMA((head_count - 1,)),
        ],
        compiler_params=pltpu.CompilerParams(collective_id=1, has_side_effects=True),
        name="reduce",
    )(dkv)


def body(queries, keys, values, grad_out, doc_ids):
    rows = queries.shape[0]
    blocks = REACH * T // rows + 1
    docs = doc_ids.reshape(rows // HD, HD)
    kv, all_docs = gather(keys, values, docs, blocks)
    attn_out, grad_queries, dkv = attend(queries, grad_out, kv, all_docs)
    grad_keys, grad_values = reduce(dkv, lax.axis_size("head"))
    return attn_out, grad_queries, grad_keys, grad_values


def solution(mesh):
    return jax.shard_map(
        body,
        mesh=mesh,
        in_specs=(P("tok", "head"), P("tok", None), P("tok", None), P("tok", "head"), P("tok")),
        out_specs=(
            P("tok", "head"),
            P("tok", "head"),
            P(("tok", "head"), None),
            P(("tok", "head"), None),
        ),
        check_vma=False,
    )
```

```python
import math

import jax
import jax.numpy as jnp
from jax import lax
from jax.experimental import pallas as pl
from jax.experimental.pallas import tpu as pltpu
from jax.sharding import PartitionSpec as P

KVH = 8
HD = 128
T = 256
REACH = 8
NT = REACH + 1
GROUPS = [(j, min(2, NT - j)) for j in range(0, NT, 2)]
BIG = -131072.0
SCALE = HD**-0.5
EXP2_SCALE = SCALE * math.log2(math.e)
NEG = -1e30


def nt(a, b):
    return lax.dot_general(a, b, (((1,), (1,)), ((), ())), preferred_element_type=jnp.float32)


def nn(a, b):
    return lax.dot_general(a, b, (((1,), (0,)), ((), ())), preferred_element_type=jnp.float32)


def attend_kernel(
    q_ref, g_ref, kv_ref, docs_ref,
    out_ref, dq_ref, dkv_ref,
    ke_ref, kt_ref, v_ref, vt_ref, bt_ref, s_ref, p_ref, dk_ref, dv_ref,
    top_ref, total_ref, ot_ref, dqt_ref,
):
    tiles = ke_ref.shape[0]
    per_block = kv_ref.shape[1] // T
    heads = q_ref.shape[1] // HD
    units = (q_ref.shape[0] // T) * heads
    half = T // HD
    kinds = lax.broadcasted_iota(jnp.int32, (HD, HD), 0)

    def prepare(i, _):
        block = i // per_block
        part = i % per_block
        rows = pl.ds(pl.multiple_of(part * T, T), T)
        key = kv_ref[block, rows, 0:HD]
        value = kv_ref[block, rows, HD : 2 * HD]
        kt_ref[i] = key.T
        vt_ref[i] = value.T
        v_ref[i] = value
        ke_ref[i, :, 0:HD] = key
        for r in range(half):
            docs = docs_ref[block, pl.ds(part * half + r, 1), :]
            hot = jnp.where(docs == kinds, 1.0, 0.0)
            ke_ref[i, r * HD : (r + 1) * HD, HD : 2 * HD] = hot.T.astype(jnp.bfloat16)
        dk_ref[i] = jnp.zeros((T, HD), jnp.float32)
        dv_ref[i] = jnp.zeros((T, HD), jnp.float32)
        return 0

    lax.fori_loop(0, tiles, prepare, 0)
    dqt_ref[...] = jnp.zeros(dqt_ref.shape, jnp.float32)
    last = kv_ref.shape[0] - 1
    for r in range(per_block * half):
        docs = docs_ref[last, r : r + 1, :]
        cold = jnp.where(docs == kinds, 0.0, BIG).astype(jnp.bfloat16)
        bt_ref[r // half, :, (r % half) * HD : (r % half + 1) * HD] = cold

    key_pos = lax.broadcasted_iota(jnp.int32, (T, T), 0)
    row_pos = lax.broadcasted_iota(jnp.int32, (T, T), 1)

    def place(i):
        rb = i // heads
        h = i % heads
        return rb, pl.ds(pl.multiple_of(rb * T, T), T), pl.ds(pl.multiple_of(h * HD, HD), HD)

    def flush(i):
        _, rows, cols = place(i)
        dq_ref[rows, cols] = (dqt_ref[...] * SCALE).T.astype(jnp.bfloat16)

    def stage(a, b, c, flush_before):
        if flush_before is not None:
            flush(flush_before)
        if a is not None:
            ra, rows, cols = place(a)
            q = q_ref[rows, cols]
            inverse = 1.0 / jnp.sum(total_ref[...], axis=0, keepdims=True)
            ot = ot_ref[...] * inverse
            out_ref[rows, cols] = ot.T.astype(jnp.bfloat16)
            gn = (g_ref[rows, cols].T.astype(jnp.float32) * inverse).astype(jnp.bfloat16)
            delta = jnp.sum(gn.astype(jnp.float32) * ot, axis=0, keepdims=True)
            gr = gn.T
            dqt = jnp.zeros((HD, T), jnp.float32)
        if b is not None:
            rb, _, _ = place(b)
            top = jnp.max(top_ref[...], axis=0, keepdims=True) * EXP2_SCALE
            total = jnp.zeros((8, T), jnp.float32)
            acc = jnp.zeros((HD, T), jnp.float32)
        if c is not None:
            rc, rows_c, cols_c = place(c)
            qt = jnp.concatenate([q_ref[rows_c, cols_c].T, bt_ref[rc]], axis=0)
            peak = jnp.full((8, T), NEG, jnp.float32)
        def scores():
            return nn(ke_ref[pl.ds(rc + j, n)].reshape(n * T, 2 * HD), qt)

        def slopes():
            return nn(v_ref[pl.ds(ra + j, n)].reshape(n * T, HD), gn)

        for j, n in GROUPS:
            if a is not None:
                pa = p_ref[j : j + n].reshape(n * T, T)
                if j > 0:
                    dp = slopes()
            if b is not None:
                old = s_ref[j : j + n].reshape(n * T, T)
            if c is not None:
                s = scores()
            if a is not None and j > 0:
                dv_ref[pl.ds(ra + j, n)] += nn(pa, gr).reshape(n, T, HD)
            if b is not None:
                p = jnp.exp2(old * EXP2_SCALE - top)
                total = total + jnp.sum(p.reshape(n * T // 8, 8, T), axis=0)
                pb = p.astype(jnp.bfloat16)
                p_ref[j : j + n] = pb.reshape(n, T, T)
                for m in range(n):
                    acc = acc + nn(vt_ref[rb + j + m], pb[m * T : (m + 1) * T])
            if a is not None and j == 0:
                dp = slopes()
                dv_ref[pl.ds(ra + j, n)] += nn(pa, gr).reshape(n, T, HD)
            if c is not None:
                s = s.reshape(n, T, T)
                for m in range(n):
                    piece = s[m]
                    if j + m == NT - 1:
                        piece = jnp.where(key_pos <= row_pos, piece, BIG)
                    s_ref[j + m] = piece
                    peak = jnp.maximum(peak, jnp.max(piece.reshape(T // 8, 8, T), axis=0))
            if a is not None:
                ds = (dp - delta).astype(jnp.bfloat16) * pa
                for m in range(n):
                    dqt = dqt + nn(kt_ref[ra + j + m], ds[m * T : (m + 1) * T])
                dk_ref[pl.ds(ra + j, n)] += nn(ds, q).reshape(n, T, HD)
        if a is not None:
            dqt_ref[...] = dqt
        if b is not None:
            total_ref[...] = total
            ot_ref[...] = acc
        if c is not None:
            top_ref[...] = peak

    stage(None, None, 0, None)
    stage(None, 0, 1, None)

    def main(i, _):
        stage(i, i + 1, i + 2, jnp.maximum(i - 1, 0))
        return 0

    lax.fori_loop(0, units - 2, main, 0)
    stage(units - 2, units - 1, None, units - 3)
    stage(units - 1, None, None, units - 2)
    flush(units - 1)

    def finish(i, _):
        rows = pl.ds(pl.multiple_of((i % per_block) * T, T), T)
        dkv_ref[i // per_block, rows, 0:HD] = (dk_ref[i] * SCALE).astype(jnp.bfloat16)
        dkv_ref[i // per_block, rows, HD : 2 * HD] = dv_ref[i].astype(jnp.bfloat16)
        return 0

    lax.fori_loop(0, tiles, finish, 0)


def attend(q, g, kv, docs):
    blocks, rows, _ = kv.shape
    tiles = blocks * rows // T
    width = q.shape[1]
    pairs = (rows // T) * NT * T * T * (width // HD)
    return pl.pallas_call(
        attend_kernel,
        out_shape=(
            jax.ShapeDtypeStruct((rows, width), jnp.bfloat16),
            jax.ShapeDtypeStruct((rows, width), jnp.bfloat16),
            jax.ShapeDtypeStruct((blocks, rows, 2 * HD), jnp.bfloat16),
        ),
        in_specs=[pl.BlockSpec(memory_space=pltpu.VMEM)] * 4,
        out_specs=[pl.BlockSpec(memory_space=pltpu.VMEM)] * 3,
        scratch_shapes=[
            pltpu.VMEM((tiles, T, 2 * HD), jnp.bfloat16),
            pltpu.VMEM((tiles, HD, T), jnp.bfloat16),
            pltpu.VMEM((tiles, T, HD), jnp.bfloat16),
            pltpu.VMEM((tiles, HD, T), jnp.bfloat16),
            pltpu.VMEM((rows // T, HD, T), jnp.bfloat16),
            pltpu.VMEM((NT, T, T), jnp.float32),
            pltpu.VMEM((NT, T, T), jnp.bfloat16),
            pltpu.VMEM((tiles, T, HD), jnp.float32),
            pltpu.VMEM((tiles, T, HD), jnp.float32),
            pltpu.VMEM((8, T), jnp.float32),
            pltpu.VMEM((8, T), jnp.float32),
            pltpu.VMEM((HD, T), jnp.float32),
            pltpu.VMEM((HD, T), jnp.float32),
        ],
        compiler_params=pltpu.CompilerParams(vmem_limit_bytes=48 * 1024 * 1024),
        cost_estimate=pl.CostEstimate(
            flops=pairs * 12 * HD, bytes_accessed=rows * width * 8, transcendentals=pairs
        ),
        name="attend",
    )(q, g, kv, docs)


def greet(peers):
    barrier = pltpu.get_barrier_semaphore()
    for peer in peers:
        pl.semaphore_signal(
            barrier, inc=1, device_id=peer, device_id_type=pl.DeviceIdType.MESH
        )
    pl.semaphore_wait(barrier, len(peers))


def others(axis):
    count = lax.axis_size(axis)
    me = lax.axis_index(axis)
    return [{axis: lax.rem(me + d, count)} for d in range(1, count)]


def gather_kernel(
    keys_ref, values_ref, docs_ref, kv_ref, all_docs_ref, load_sems, send_sems, recv_sems
):
    tok = lax.axis_index("tok")
    toks = lax.axis_size("tok")
    group = lax.axis_index("head") // (lax.axis_size("head") // KVH)
    blocks = kv_ref.shape[0]
    last = blocks - 1
    cols = pl.ds(pl.multiple_of(group * HD, HD), HD)
    loads = [
        pltpu.make_async_copy(keys_ref.at[:, cols], kv_ref.at[last, :, 0:HD], load_sems.at[0]),
        pltpu.make_async_copy(
            values_ref.at[:, cols], kv_ref.at[last, :, HD : 2 * HD], load_sems.at[1]
        ),
    ]
    for load in loads:
        load.start()
    all_docs_ref[last] = docs_ref[...]
    greet(others("tok"))
    for load in loads:
        load.wait()

    def copies(d, peer):
        return [
            pltpu.make_async_remote_copy(
                src_ref=kv_ref.at[last],
                dst_ref=kv_ref.at[last - d],
                send_sem=send_sems.at[0, d - 1],
                recv_sem=recv_sems.at[0, d - 1],
                device_id={"tok": peer},
                device_id_type=pl.DeviceIdType.MESH,
            ),
            pltpu.make_async_remote_copy(
                src_ref=docs_ref,
                dst_ref=all_docs_ref.at[last - d],
                send_sem=send_sems.at[1, d - 1],
                recv_sem=recv_sems.at[1, d - 1],
                device_id={"tok": peer},
                device_id_type=pl.DeviceIdType.MESH,
            ),
        ]

    for d in range(1, blocks):

        @pl.when(tok + d < toks)
        def _():
            for copy in copies(d, tok + d):
                copy.start()

        @pl.when(tok < d)
        def _():
            kv_ref[last - d] = jnp.zeros(kv_ref.shape[1:], jnp.bfloat16)
            all_docs_ref[last - d] = jnp.full(docs_ref.shape, 6, jnp.int32)

    for d in range(1, blocks):

        @pl.when(tok + d < toks)
        def _():
            for copy in copies(d, tok + d):
                copy.wait_send()

        @pl.when(tok >= d)
        def _():
            for copy in copies(d, tok - d):
                copy.wait_recv()


def gather(keys, values, docs, blocks):
    rows = keys.shape[0]
    vmem = pl.BlockSpec(memory_space=pltpu.VMEM)
    hbm = pl.BlockSpec(memory_space=pl.ANY)
    return pl.pallas_call(
        gather_kernel,
        out_shape=(
            jax.ShapeDtypeStruct((blocks, rows, 2 * HD), jnp.bfloat16),
            jax.ShapeDtypeStruct((blocks,) + docs.shape, jnp.int32),
        ),
        in_specs=[hbm, hbm, vmem],
        out_specs=[vmem, vmem],
        scratch_shapes=[
            pltpu.SemaphoreType.DMA((2,)),
            pltpu.SemaphoreType.DMA((2, blocks - 1)),
            pltpu.SemaphoreType.DMA((2, blocks - 1)),
        ],
        compiler_params=pltpu.CompilerParams(collective_id=0, has_side_effects=True),
        name="gather",
    )(keys, values, docs)


def reduce_kernel(
    dkv_ref, dk_ref, dv_ref, terms_ref, mid_ref, parts_ref, send_sems, recv_sems, out_sems, in_sems
):
    tok = lax.axis_index("tok")
    toks = lax.axis_size("tok")
    head = lax.axis_index("head")
    head_count = lax.axis_size("head")
    blocks = dkv_ref.shape[0]
    last = blocks - 1
    piece = mid_ref.shape[1]
    greet(others("tok") + others("head"))

    def term(d, peer):
        return pltpu.make_async_remote_copy(
            src_ref=dkv_ref.at[last - d],
            dst_ref=terms_ref.at[d - 1],
            send_sem=send_sems.at[d - 1],
            recv_sem=recv_sems.at[d - 1],
            device_id={"tok": peer},
            device_id_type=pl.DeviceIdType.MESH,
        )

    for d in range(1, blocks):

        @pl.when(tok >= d)
        def _():
            term(d, tok - d).start()

        @pl.when(tok + d >= toks)
        def _():
            terms_ref[d - 1] = jnp.zeros(terms_ref.shape[1:], jnp.bfloat16)

    for d in range(1, blocks):

        @pl.when(tok + d < toks)
        def _():
            term(d, tok + d).wait_recv()

    def add(i, _):
        rows = pl.ds(pl.multiple_of(i * piece, piece), piece)
        total = dkv_ref[last, rows, :].astype(jnp.float32)
        for d in range(1, blocks):
            total = total + terms_ref[d - 1, rows, :].astype(jnp.float32)
        mid_ref[i] = total.astype(jnp.bfloat16)
        return 0

    lax.fori_loop(0, head_count, add, 0)

    def part(d, peer, slot):
        return pltpu.make_async_remote_copy(
            src_ref=mid_ref.at[peer],
            dst_ref=parts_ref.at[slot],
            send_sem=out_sems.at[d - 1],
            recv_sem=in_sems.at[d - 1],
            device_id={"head": peer},
            device_id_type=pl.DeviceIdType.MESH,
        )

    for d in range(1, head_count):
        part(d, lax.rem(head + d, head_count), head).start()
    parts_ref[head] = mid_ref[head]
    for d in range(1, head_count):
        source = lax.rem(head + head_count - d, head_count)
        part(d, source, source).wait_recv()
    copies = head_count // KVH
    for g in range(KVH):
        total = parts_ref[g * copies].astype(jnp.float32)
        for c in range(1, copies):
            total = total + parts_ref[g * copies + c].astype(jnp.float32)
        total = total.astype(jnp.bfloat16)
        dk_ref[:, g * HD : (g + 1) * HD] = total[:, 0:HD]
        dv_ref[:, g * HD : (g + 1) * HD] = total[:, HD : 2 * HD]
    for d in range(1, blocks):

        @pl.when(tok >= d)
        def _():
            term(d, tok - d).wait_send()

    for d in range(1, head_count):
        part(d, lax.rem(head + d, head_count), head).wait_send()


def reduce(dkv, head_count):
    blocks, rows, width = dkv.shape
    piece = rows // head_count
    vmem = pl.BlockSpec(memory_space=pltpu.VMEM)
    return pl.pallas_call(
        reduce_kernel,
        out_shape=(jax.ShapeDtypeStruct((piece, KVH * HD), jnp.bfloat16),) * 2,
        in_specs=[vmem],
        out_specs=[vmem, vmem],
        scratch_shapes=[
            pltpu.VMEM((blocks - 1, rows, width), jnp.bfloat16),
            pltpu.VMEM((head_count, piece, width), jnp.bfloat16),
            pltpu.VMEM((head_count, piece, width), jnp.bfloat16),
            pltpu.SemaphoreType.DMA((blocks - 1,)),
            pltpu.SemaphoreType.DMA((blocks - 1,)),
            pltpu.SemaphoreType.DMA((head_count - 1,)),
            pltpu.SemaphoreType.DMA((head_count - 1,)),
        ],
        compiler_params=pltpu.CompilerParams(collective_id=1, has_side_effects=True),
        name="reduce",
    )(dkv)


def body(queries, keys, values, grad_out, doc_ids):
    rows = queries.shape[0]
    blocks = REACH * T // rows + 1
    docs = doc_ids.reshape(rows // HD, HD)
    kv, all_docs = gather(keys, values, docs, blocks)
    attn_out, grad_queries, dkv = attend(queries, grad_out, kv, all_docs)
    grad_keys, grad_values = reduce(dkv, lax.axis_size("head"))
    return attn_out, grad_queries, grad_keys, grad_values


def solution(mesh):
    return jax.shard_map(
        body,
        mesh=mesh,
        in_specs=(P("tok", "head"), P("tok", None), P("tok", None), P("tok", "head"), P("tok")),
        out_specs=(
            P("tok", "head"),
            P("tok", "head"),
            P(("tok", "head"), None),
            P(("tok", "head"), None),
        ),
        check_vma=False,
    )
```
